256 devices in a mesh: row: 16 (over z, x_lo), col: 16 (over x_hi, y, core).
Axes of the slice: x: 4 (x_hi: 2, x_lo: 2; x = x_hi * 2 + x_lo), y: 4, z: 8, core: 2. Of those that a mesh axis runs over, the one named last changes fastest.
Arguments:
- tiles: bfloat16 [16, 16, 3, 256, 256], P('row', 'col'), as said below
- stack_index: int32 [16, 16, 3], P('row', 'col'), may hold values from 0 to 15, as said below
- block_mask: int32 [64, 64], replicated, may hold values from 0 to 1, as said below
Outputs:
- purified: bfloat16 [16, 16, 3, 256, 256], P('row', 'col')
The draws below stay inside these ranges and needn't reach their ends.
Inputs may be any that keep to these rules, and one draw needn't show every extreme that they name: `block_mask`: the region of one device (4 x 4 blocks) holds at most 3 occupied blocks; some region holds exactly 3 in every draw. `stack_index`: block (a, b) of a device's region is numbered a * 4 + b. A device's 3 entries are distinct and include every occupied block of its region; a slot naming an unoccupied block holds a tile that P does not use. `tiles`: A slot's tile is P's block named by stack_index when that block is occupied.
All inputs are finite; a program needn't handle non-finite values.
Results may differ from the reference program's by a relative error of at most 0.0051.
Values may be sent and summed in bfloat16 or wider, within the bound.
No kernel may reach another device: no remote copies, remote signals or barrier semaphores. Data moves between devices by JAX's collectives and lax.ppermute only.
A program may use at most 64 MiB of HBM per device.

```python
import jax
import jax.numpy as jnp
from jax import lax

NB = 64
BS = 256
SLOTS = 3
BR = 4
BC = 4
N_ROW = 16
N_COL = 16


def to_regions(table):
    return table.reshape(N_ROW, BR, N_COL, BC).transpose(0, 2, 1, 3).reshape(N_ROW, N_COL, BR * BC)


def block_layout(key):
    cluster_key = jax.random.fold_in(key, 301)
    anchor_row_key = jax.random.fold_in(key, 302)
    anchor_col_key = jax.random.fold_in(key, 303)
    noise_key = jax.random.fold_in(key, 304)
    mixing_key = jax.random.fold_in(key, 305)
    cluster = jax.random.randint(cluster_key, (NB,), 0, max(NB // 8, 1), dtype=jnp.int32)
    row_iota = jnp.arange(NB, dtype=jnp.int32)[:, None]
    col_iota = jnp.arange(NB, dtype=jnp.int32)[None, :]
    anchor_row = jax.random.randint(anchor_row_key, (), 0, N_ROW, dtype=jnp.int32)
    anchor_col = jax.random.randint(anchor_col_key, (), 0, N_COL, dtype=jnp.int32)
    favoured = (row_iota // BR == anchor_row) & (col_iota // BC == anchor_col)
    candidate = ((cluster[:, None] == cluster[None, :]) | favoured).astype(jnp.int32)
    noise_draw = jax.random.randint(noise_key, (NB, NB), 0, 1024, dtype=jnp.int32)
    priority = candidate * 4096 + noise_draw
    local_count = BR * BC
    local_iota = jnp.arange(local_count, dtype=jnp.int32)
    region_priority = to_regions(priority) * local_count + local_iota
    _, picked = lax.top_k(region_priority, SLOTS)
    picked = picked.astype(jnp.int32)
    kept_slot = jnp.sum((picked[:, :, :, None] == local_iota[None, None, None, :]).astype(jnp.int32), axis=2)
    region_mask = to_regions(candidate) * kept_slot
    occupied = region_mask.reshape(N_ROW, N_COL, BR, BC).transpose(0, 2, 1, 3).reshape(NB, NB)
    mixing = jax.random.randint(mixing_key, (N_ROW, N_COL, SLOTS), 0, 4096, dtype=jnp.int32) * SLOTS + jnp.arange(SLOTS, dtype=jnp.int32)
    placement = jnp.argsort(mixing, axis=2)
    stack_ids = jnp.take_along_axis(picked, placement, axis=2)
    return (occupied, stack_ids)


def draw_block_mask(key, part):
    return block_layout(key)[0]


def draw_stack_index(key, part):
    return block_layout(key)[1]


def draw_tiles(key, part):
    occupied, stack_ids = block_layout(key)
    noise_key = jax.random.fold_in(key, 201)
    tile_shape = (N_ROW, N_COL, SLOTS, BS, BS)
    spread = 1.0 / BS ** 0.5
    noise_draw = spread * jax.random.normal(noise_key, tile_shape, jnp.float32)
    band_row = jnp.arange(N_ROW, dtype=jnp.int32)[:, None, None]
    band_col = jnp.arange(N_COL, dtype=jnp.int32)[None, :, None]
    on_diagonal = band_row * BR + stack_ids // BC == band_col * BC + stack_ids % BC
    identity = jnp.eye(BS, dtype=jnp.float32)
    values = noise_draw + 0.5 * on_diagonal.astype(jnp.float32)[:, :, :, None, None] * identity
    return values.astype(jnp.bfloat16)


def setup_inputs(seed: int = 0) -> dict:
    key_of = jax.random.split(jax.random.key(seed), 4)
    return {
        "tiles": draw_tiles(jax.random.fold_in(key_of[3], 71), 0),
        "stack_index": draw_stack_index(jax.random.fold_in(key_of[3], 71), 0),
        "block_mask": draw_block_mask(jax.random.fold_in(key_of[3], 71), 0),
    }


def reference(tiles, stack_index, block_mask):
    total_slots = N_ROW * N_COL * SLOTS
    flat_tiles = tiles.reshape(total_slots, BS, BS)
    places = jnp.arange(total_slots, dtype=jnp.int32)
    device_id = places // SLOTS
    device_row = device_id // N_COL
    device_col = device_id % N_COL
    flat_ids = stack_index.reshape(total_slots).astype(jnp.int32)
    global_row = (device_row * BR + flat_ids // BC).astype(jnp.int32)
    global_col = (device_col * BC + flat_ids % BC).astype(jnp.int32)
    valid = block_mask[global_row, global_col] > 0
    slot_of = jnp.zeros((NB, NB), jnp.int32).at[global_row, global_col].set(places)

    def product(left_flat, right_flat):
        def per_slot(columns):
            block_row, block_col, live = columns

            def compute(unused):
                def inner(inner_block, total):
                    weight = block_mask[block_row, inner_block] * block_mask[inner_block, block_col]

                    def add_term(running):
                        left_tile = left_flat[slot_of[block_row, inner_block]]
                        right_tile = right_flat[slot_of[inner_block, block_col]]
                        return running + jnp.dot(left_tile, right_tile, preferred_element_type=jnp.float32)

                    def keep_term(running):
                        return running

                    return lax.cond(weight > 0, add_term, keep_term, total)

                return lax.fori_loop(0, NB, inner, jnp.zeros((BS, BS), jnp.float32))

            def skipped(unused):
                return jnp.zeros((BS, BS), jnp.float32)

            return lax.cond(live, compute, skipped, 0)

        return lax.map(per_slot, (global_row, global_col, valid))

    square = product(flat_tiles, flat_tiles).astype(jnp.bfloat16)
    cube_sum = product(square, flat_tiles)
    valid_float = valid.astype(jnp.float32)
    purified = (3.0 * square.astype(jnp.float32) - 2.0 * cube_sum) * valid_float[:, None, None]
    return purified.astype(jnp.bfloat16).reshape(N_ROW, N_COL, SLOTS, BS, BS)
```

```python
import jax
import jax.numpy as jnp
from jax import lax
from jax.experimental import pallas as pl
from jax.experimental.pallas import tpu as pltpu
from jax.sharding import PartitionSpec as P

NB = 64
BS = 256
SLOTS = 3
HALF = BS // 2
I32 = jnp.int32


def links():
    def table(move):
        pairs = []
        for z in range(8):
            for a in range(2):
                for b in range(2):
                    for y in range(4):
                        for c in range(2):
                            z2, a2, b2, y2, c2 = move(z, a, b, y, c)
                            here = (z * 2 + a) * 16 + b * 8 + y * 2 + c
                            there = (z2 % 8 * 2 + a2) * 16 + b2 * 8 + y2 % 4 * 2 + c2
                            pairs.append((here, there))
        return pairs

    def across(z, a, b, y, c):
        x = (b * 2 + a + (1 if a == 1 else -1)) % 4
        return z, x % 2, x // 2, y, c

    return {
        "z+": table(lambda z, a, b, y, c: (z - 1, a, b, y, c)),
        "z-": table(lambda z, a, b, y, c: (z + 1, a, b, y, c)),
        "y+": table(lambda z, a, b, y, c: (z, a, b, y - 1, c)),
        "y-": table(lambda z, a, b, y, c: (z, a, b, y + 1, c)),
        "xl": table(lambda z, a, b, y, c: (z, 1 - a, b, y, c)),
        "xr": table(across),
        "xh": table(lambda z, a, b, y, c: (z, a, 1 - b, y, c)),
        "core": table(lambda z, a, b, y, c: (z, a, b, y, 1 - c)),
    }


LINKS = links()


def send(part, link):
    return lax.ppermute(part, ("row", "col"), LINKS[link])


def gather_rows(own):
    partner = send(own, "xl")
    pieces = []
    for base, seed in ((0, own), (8, partner)):
        up, down = seed, seed
        pieces.append((base, 0, seed))
        for step in range(1, 4):
            up, down = send(up, "z+"), send(down, "z-")
            pieces += [(base + step, 0, up), (base + 8 - step, 0, down)]
        pieces.append((base + 4, 0, send(up[:, :HALF], "z+")))
        pieces.append((base + 4, HALF, send(down[:, HALF:], "z-")))
    return pieces, partner


def gather_cols(own, other):
    pieces = []
    for base, seed in ((0, own), (4, other)):
        up, down = send(seed, "y+"), send(seed, "y-")
        pieces += [(base, 0, seed), (base + 1, 0, up), (base + 3, 0, down)]
        pieces.append((base + 2, 0, send(up[:, :HALF], "y+")))
        pieces.append((base + 2, HALF, send(down[:, HALF:], "y-")))
    return pieces + [(place + 8, first, send(part, "core")) for place, first, part in pieces]


def plan(ids, mask):
    r, c = lax.axis_index("row"), lax.axis_index("col")
    rows = lax.dynamic_slice(mask, (4 * r, 0), (4, NB)) > 0
    cols = lax.dynamic_slice(mask, (0, 4 * c), (NB, 4)) > 0
    here = lax.dynamic_slice(mask, (4 * r, 4 * c), (4, 4)) > 0
    a4, b4 = jnp.arange(4, dtype=I32)[:, None], jnp.arange(4, dtype=I32)[None, :]
    live = jnp.sum((here & (a4 * 4 + b4 == ids[:, None, None])).astype(I32), axis=(1, 2)) > 0
    slot = jnp.arange(SLOTS, dtype=I32)
    key = jnp.where(live, ids, 16 + slot)
    rank = jnp.sum((key[None, :] < key[:, None]).astype(I32), axis=1)
    pick = (rank[None, :] == slot[:, None]).astype(I32)
    order = jnp.sum(pick * slot[None, :], axis=1)
    block = jnp.sum(pick * ids[None, :], axis=1)
    valid = jnp.sum(pick * live.astype(I32)[None, :], axis=1) > 0
    own_a, own_b = block // 4, block % 4

    k = jnp.arange(NB, dtype=I32)
    region, inner = k // 4, k % 4
    same = region[:, None] == region[None, :]
    four = jnp.arange(4, dtype=I32)
    before_left = (
        rows[None, None, :, :]
        & same[None, :, None, :]
        & (four[None, None, :, None] * 4 + inner[None, None, None, :] < own_a[:, None, None, None] * 4 + inner[None, :, None, None])
    )
    left_slot = jnp.sum(before_left.astype(I32), axis=(2, 3))
    before_right = (
        cols.T[None, None, :, :]
        & same[None, :, None, :]
        & (inner[None, None, None, :] * 4 + four[None, None, :, None] < inner[None, :, None, None] * 4 + own_b[:, None, None, None])
    )
    right_slot = jnp.sum(before_right.astype(I32), axis=(2, 3))
    left_has = jnp.sum((rows[None, :, :] & (four[None, :, None] == own_a[:, None, None])).astype(I32), axis=1) > 0
    right_has = jnp.sum((cols.T[None, :, :] & (four[None, :, None] == own_b[:, None, None])).astype(I32), axis=1) > 0
    term = left_has & right_has & valid[:, None]
    left_place = ((region // 2 - c // 2) % 4) + 4 * (region // 8 != c // 8) + 8 * (region % 2 != c % 2)
    right_place = ((region // 2 - r // 2) % 8) + 8 * (region % 2 != r % 2)
    left = left_place[None, :] * SLOTS + left_slot
    right = right_place[None, :] * SLOTS + right_slot

    at = jnp.sum((term[:, None, :] & (k[None, None, :] < k[None, :, None])).astype(I32), axis=2)
    hit = term[:, None, :] & (at[:, None, :] == k[None, :, None])
    code = left * 64 + right
    spare = 16 * SLOTS * 65
    pairs = jnp.sum(jnp.where(hit, code[:, None, :] - spare, 0), axis=2) + spare
    count = jnp.sum(term.astype(I32), axis=1)
    tile = jnp.arange(16 * SLOTS, dtype=I32)
    need_left = jnp.sum((term[:, :, None] & (left[:, :, None] == tile)).astype(I32), axis=(0, 1))
    need_right = jnp.sum((term[:, :, None] & (right[:, :, None] == tile)).astype(I32), axis=(0, 1))
    return order, pairs, count, need_left, need_right


def multiply(pairs, count, need_left, need_right, order, left, right, square=None):
    left_at = [(place, first) for place, first, _ in left]
    right_at = [(place, first) for place, first, _ in right]
    n_left, n_right = len(left), len(right)

    def body(pairs_ref, count_ref, nl_ref, nr_ref, order_ref, *refs):
        left_refs, right_refs = refs[:n_left], refs[n_left : n_left + n_right]
        rest = refs[n_left + n_right :]
        if square is None:
            out_ref, lbuf, rbuf, total = rest
        else:
            square_ref, out_ref, lbuf, rbuf, total = rest

        for need, places, sources, buf in ((nl_ref, left_at, left_refs, lbuf), (nr_ref, right_at, right_refs, rbuf)):
            buf[16 * SLOTS] = jnp.zeros((BS, BS), jnp.bfloat16)
            for (place, first), source in zip(places, sources):
                for s in range(SLOTS):
                    t = place * SLOTS + s

                    @pl.when(need[t] > 0)
                    def _():
                        buf[t, pl.ds(first, source.shape[1])] = source[s]

        for s in range(SLOTS):
            total[...] = jnp.zeros_like(total)

            def step(p, _):
                one, two = pairs_ref[s, 2 * p], pairs_ref[s, 2 * p + 1]
                total[...] += jnp.dot(
                    lbuf[one // 64], rbuf[one % 64], preferred_element_type=jnp.float32
                ) + jnp.dot(lbuf[two // 64], rbuf[two % 64], preferred_element_type=jnp.float32)
                return 0

            lax.fori_loop(0, (count_ref[s] + 1) // 2, step, 0)
            if square is None:
                out_ref[s] = total[...].astype(jnp.bfloat16)
            else:
                out_ref[order_ref[s]] = (3.0 * square_ref[s].astype(jnp.float32) - 2.0 * total[...]).astype(jnp.bfloat16)

    smem = pl.BlockSpec(memory_space=pltpu.SMEM)
    vmem = pl.BlockSpec(memory_space=pltpu.VMEM)
    extra = [] if square is None else [square]
    return pl.pallas_call(
        body,
        out_shape=jax.ShapeDtypeStruct((SLOTS, BS, BS), jnp.bfloat16),
        in_specs=[smem] * 5 + [vmem] * (n_left + n_right) + [vmem] * len(extra),
        out_specs=vmem,
        scratch_shapes=[
            pltpu.VMEM((16 * SLOTS + 1, BS, BS), jnp.bfloat16),
            pltpu.VMEM((16 * SLOTS + 1, BS, BS), jnp.bfloat16),
            pltpu.VMEM((BS, BS), jnp.float32),
        ],
        compiler_params=pltpu.CompilerParams(vmem_limit_bytes=32 * 1024 * 1024),
        name="square" if square is None else "cube",
    )(pairs, count, need_left, need_right, order, *(a for _, _, a in left), *(a for _, _, a in right), *extra)


def local(tiles, stack_index, block_mask):
    order, pairs, count, need_left, need_right = plan(stack_index[0, 0], block_mask)
    own = jnp.take(tiles[0, 0], order, axis=0)
    right, partner = gather_rows(own)
    left = gather_cols(own, send(partner, "xr"))
    square = multiply(pairs, count, need_left, need_right, order, left, right)
    left = gather_cols(square, send(square, "xh"))
    purified = multiply(pairs, count, need_left, need_right, order, left, right, square)
    return purified[None, None]


def solution(mesh):
    return jax.shard_map(
        local,
        mesh=mesh,
        in_specs=(P("row", "col", None, None, None), P("row", "col", None), P()),
        out_specs=P("row", "col", None, None, None),
        check_vma=False,
    )
```

```python
import jax
import jax.numpy as jnp
from jax import lax
from jax.experimental import pallas as pl
from jax.experimental.pallas import tpu as pltpu
from jax.sharding import PartitionSpec as P


NB = 64
BS = 256
SLOTS = 3
I32 = jnp.int32


def links():
    def table(move):
        pairs = []
        for z in range(8):
            for a in range(2):
                for b in range(2):
                    for y in range(4):
                        for c in range(2):
                            z2, a2, b2, y2, c2 = move(z, a, b, y, c)
                            here = (z * 2 + a) * 16 + b * 8 + y * 2 + c
                            there = (z2 % 8 * 2 + a2) * 16 + b2 * 8 + y2 % 4 * 2 + c2
                            pairs.append((here, there))
        return pairs

    def across(z, a, b, y, c):
        x = (b * 2 + a + (1 if a == 1 else -1)) % 4
        return z, x % 2, x // 2, y, c

    return {
        "z+": table(lambda z, a, b, y, c: (z - 1, a, b, y, c)),
        "z-": table(lambda z, a, b, y, c: (z + 1, a, b, y, c)),
        "y": table(lambda z, a, b, y, c: (z, a, b, y + (1 if c else -1), c)),
        "y2": table(lambda z, a, b, y, c: (z, a, b, y + 2, c)),
        "xl": table(lambda z, a, b, y, c: (z, 1 - a, b, y, c)),
        "xr": table(across),
        "xh": table(lambda z, a, b, y, c: (z, a, 1 - b, y, c)),
        "core": table(lambda z, a, b, y, c: (z, a, b, y, 1 - c)),
    }


LINKS = links()


def send(part, link):
    return lax.ppermute(part, ("row", "col"), LINKS[link])


LATE_ROWS = 1 << 11 | 1 << 12 | 1 << 13
LATE_COLS_FIRST = 1 << 14
LATE_COLS_SECOND = 1 << 9 | 1 << 11 | 1 << 13 | 1 << 15
STRIDE = 72
SPARE = SLOTS * 16
COUNTS = 4 * SLOTS * STRIDE
ORDERS = COUNTS + 16


def gather_rows(own):
    down1, up1 = send(own, "z-"), send(own, "z+")
    partner = send(own, "xl")
    down2, up2 = send(down1, "z-"), send(up1, "z+")
    across7, across1 = send(down1, "xl"), send(up1, "xl")
    down3, up3 = send(down2, "z-"), send(up2, "z+")
    across2, across6 = send(up2, "xl"), send(across7, "z-")
    up4 = send(up3, "z+")
    across5, across3 = send(across6, "z-"), send(across2, "z+")
    across4 = send(up4, "xl")
    stacks = [own, up1, up2, up3, up4, down3, down2, down1]
    stacks += [partner, across1, across2, across3, across4, across5, across6, across7]
    return [(place, 0, stack) for place, stack in enumerate(stacks)], partner


def gather_cols(own, partner=None):
    twin = send(own, "core")
    both = jnp.concatenate([own, twin])
    near = send(both, "y")
    far = send(near, "core")
    opposite = send(own, "y2")
    opposite_twin = send(opposite, "core")
    if partner is None:
        x = send(own, "xh")
        x_opposite = send(opposite, "xh")
    else:
        x = send(partner, "xr")
        x_opposite = send(x, "y2")
    x_twin = send(x, "core")
    x_both = jnp.concatenate([x, x_twin])
    x_near = send(x_both, "y")
    x_far = send(x_near, "core")
    x_opposite_twin = send(x_opposite, "core")
    return [
        (0, 0, both), (4, SLOTS, both), (1, 0, near), (5, SLOTS, near), (7, 0, far), (3, SLOTS, far),
        (2, 0, opposite), (6, 0, opposite_twin), (8, 0, x_both), (12, SLOTS, x_both), (9, 0, x_near), (13, SLOTS, x_near),
        (15, 0, x_far), (11, SLOTS, x_far), (10, 0, x_opposite), (14, 0, x_opposite_twin),
    ]


SMEM = pl.BlockSpec(memory_space=pltpu.SMEM)
VMEM = pl.BlockSpec(memory_space=pltpu.VMEM)


def small(kib):
    return pltpu.CompilerParams(vmem_limit_bytes=kib * 1024)


def arrange(tiles, ids, mask):
    def body(ids_ref, mask_ref, tiles_ref, order_ref, own_ref):
        r, c = lax.axis_index("row"), lax.axis_index("col")
        keys = []
        for s in range(SLOTS):
            block = ids_ref[s]
            live = mask_ref[4 * r + block // 4, 4 * c + block % 4] > 0
            keys.append(jnp.where(live, block, 16 + s))
        for s in range(SLOTS):
            rank = sum((keys[t] < keys[s]).astype(I32) for t in range(SLOTS) if t != s)
            order_ref[rank] = s
            order_ref[SLOTS + rank] = ids_ref[s]
            own_ref[rank] = tiles_ref[s]
        order_ref[2 * SLOTS] = sum((key < 16).astype(I32) for key in keys)

    return pl.pallas_call(
        body,
        out_shape=(jax.ShapeDtypeStruct((8,), I32), jax.ShapeDtypeStruct((SLOTS, BS, BS), jnp.bfloat16)),
        in_specs=[SMEM, SMEM, VMEM],
        out_specs=(SMEM, VMEM),
        name="arrange",
    )(ids, mask, tiles)


def tables(mask):
    def body(mask_ref, left_ref, right_ref):
        r, c = lax.axis_index("row"), lax.axis_index("col")
        toward = jnp.where(c % 2 == 0, 1, 3)
        full = (mask_ref[...] > 0).astype(jnp.bfloat16)
        sub = lax.broadcasted_iota(I32, (8, NB), 0)
        lane = lax.broadcasted_iota(I32, (8, NB), 1)

        def dot(one, two, dims):
            return lax.dot_general(one, two, (dims, ((), ())), preferred_element_type=jnp.float32)

        rows = dot(((lane == 4 * r + sub) & (sub < 4)).astype(jnp.bfloat16), full, ((1,), (0,)))
        cols = dot(((lane == 4 * c + sub) & (sub < 4)).astype(jnp.bfloat16), full, ((1,), (1,)))
        k0 = lax.broadcasted_iota(I32, (NB, NB), 0)
        k1 = lax.broadcasted_iota(I32, (NB, NB), 1)
        same = (k0 >> 2) == (k1 >> 2)
        earlier = (same & (k0 < k1)).astype(jnp.bfloat16)
        above = (lax.broadcasted_iota(I32, (8, 8), 1) < lax.broadcasted_iota(I32, (8, 8), 0)).astype(jnp.bfloat16)
        rows16, cols16 = rows.astype(jnp.bfloat16), cols.astype(jnp.bfloat16)
        row_totals = dot(rows16, same.astype(jnp.bfloat16), ((1,), (0,))).astype(jnp.bfloat16)
        left_slot = dot(rows16, earlier, ((1,), (0,))) + dot(above, row_totals, ((1,), (0,)))
        col_totals = dot(jnp.ones((8, 8), jnp.bfloat16), cols16, ((1,), (0,))).astype(jnp.bfloat16)
        right_slot = dot(col_totals, earlier, ((1,), (0,))) + dot(above, cols16, ((1,), (0,)))

        k = lane >> 2
        left = ((((k >> 1) - (c // 2) + 16) & 3) * toward & 3) + 4 * ((k ^ c) & 1) + 8 * ((k >> 3) ^ (c // 8))
        right = (((k >> 1) - (r // 2) + 8) & 7) + 8 * ((k ^ r) & 1)

        def late(places, bits):
            return sum((places == place).astype(I32) for place in range(16) if bits >> place & 1)

        left_at = left * SLOTS + 64 * late(left, LATE_COLS_FIRST) + 128 * late(left, LATE_COLS_SECOND)
        right_at = right * SLOTS + 64 * late(right, LATE_ROWS)
        left_ref[...] = jnp.where(rows > 0.5, left_at + left_slot.astype(I32), -1)
        right_ref[...] = jnp.where(cols > 0.5, right_at + right_slot.astype(I32), -1)

    return pl.pallas_call(
        body,
        out_shape=(jax.ShapeDtypeStruct((8, NB), I32), jax.ShapeDtypeStruct((8, NB), I32)),
        in_specs=[VMEM],
        out_specs=(VMEM, VMEM),
        compiler_params=small(1024),
        name="tables",
    )(mask)


def plan(left_table, right_table, order):
    def body(left_ref, right_ref, order_ref, plan_ref):
        for s in range(SLOTS):
            plan_ref[ORDERS + s] = order_ref[s]
            block = order_ref[SLOTS + s]
            a, b = block // 4, block % 4

            def term(step, counts, a=a, b=b, s=s):
                for i in range(4):
                    k = 4 * step + i
                    left, right = left_ref[a, k], right_ref[b, k]
                    one = ((left >= 0) & (right >= 0)).astype(I32)
                    code = (left & 63) * 64 + (right & 63)
                    fresh = []
                    for first, late in ((0, ((left | right) >> 6) & 1), (2, (left >> 7) & 1)):
                        at = jnp.where(late > 0, counts[first + 1] + SLOTS * STRIDE, counts[first])
                        plan_ref[(first * SLOTS + s) * STRIDE + at] = code
                        more = one & late
                        fresh += [counts[first] + (one - more), counts[first + 1] + more]
                    counts = tuple(fresh)
                return counts

            zero = jnp.int32(0)
            counts = lax.fori_loop(0, jnp.where(s < order_ref[2 * SLOTS], NB // 4, 0), term, (zero, zero, zero, zero))
            for q in range(4):
                plan_ref[COUNTS + q * 4 + s] = counts[q]
                plan_ref[(q * SLOTS + s) * STRIDE + counts[q]] = SPARE * 65

    return pl.pallas_call(
        body,
        out_shape=jax.ShapeDtypeStruct((ORDERS + 8,), I32),
        in_specs=[SMEM, SMEM, SMEM],
        out_specs=SMEM,
        compiler_params=small(1024),
        name="plan",
    )(left_table, right_table, order)


def fill(pieces, refs, buf):
    for (place, first, _), which in zip(*pieces):
        for s in range(SLOTS):
            buf[place * SLOTS + s] = refs[which][first + s]


def split(pieces):
    arrays = list({id(array): array for _, _, array in pieces}.values())
    return arrays, (pieces, [[array is a for a in arrays].index(True) for _, _, array in pieces])


def products(which_list, plan_ref, lbuf, rbuf, total, s):
    def step(p, _):
        at = (which_list * SLOTS + s) * STRIDE + 2 * p
        one, two = plan_ref[at], plan_ref[at + 1]
        total[...] += jnp.dot(lbuf[one // 64], rbuf[one % 64], preferred_element_type=jnp.float32) + jnp.dot(
            lbuf[two // 64], rbuf[two % 64], preferred_element_type=jnp.float32
        )
        return 0

    lax.fori_loop(0, (plan_ref[COUNTS + which_list * 4 + s] + 1) // 2, step, 0)


BUFFER = jax.ShapeDtypeStruct((SPARE + 1, BS, BS), jnp.bfloat16)
TOTALS = jax.ShapeDtypeStruct((SLOTS, BS, BS), jnp.float32)
STACK = jax.ShapeDtypeStruct((SLOTS, BS, BS), jnp.bfloat16)
PARAMS = pltpu.CompilerParams(vmem_limit_bytes=8 * 1024 * 1024)


def multiply_early(which_list, lists, left, right):
    left_arrays, left_pieces = split(left)
    right_arrays, right_pieces = split(right) if isinstance(right, list) else ([right], None)
    n_left = len(left_arrays)

    def body(plan_ref, *refs):
        left_refs, right_refs, outs = refs[:n_left], refs[n_left : n_left + len(right_arrays)], refs[n_left + len(right_arrays) :]
        totals, lbuf = outs[:2]
        lbuf[SPARE] = jnp.zeros((BS, BS), jnp.bfloat16)
        fill(left_pieces, left_refs, lbuf)
        if right_pieces is None:
            rbuf = right_refs[0]
        else:
            rbuf = outs[2]
            rbuf[SPARE] = jnp.zeros((BS, BS), jnp.bfloat16)
            fill(right_pieces, right_refs, rbuf)
        for s in range(SLOTS):
            totals[s] = jnp.zeros((BS, BS), jnp.float32)
            products(which_list, plan_ref, lbuf, rbuf, totals.at[s], s)

    return pl.pallas_call(
        body,
        out_shape=[TOTALS, BUFFER] + ([] if right_pieces is None else [BUFFER]),
        in_specs=[SMEM] + [VMEM] * (n_left + len(right_arrays)),
        out_specs=[VMEM] * (2 if right_pieces is None else 3),
        compiler_params=PARAMS,
    )(lists, *left_arrays, *right_arrays)


def square_late(lists, totals, lbuf, rbuf, left, right):
    left_arrays, left_pieces = split(left)
    right_arrays, right_pieces = split(right)
    n_left, n_all = len(left_arrays), len(left_arrays) + len(right_arrays)

    def body(plan_ref, *refs):
        out_ref, lbuf, rbuf, total = refs[n_all + 3 :]
        fill(left_pieces, refs[:n_left], lbuf)
        fill(right_pieces, refs[n_left:n_all], rbuf)
        for s in range(SLOTS):
            products(1, plan_ref, lbuf, rbuf, total.at[s], s)
            out_ref[s] = total[s].astype(jnp.bfloat16)

    out = pl.pallas_call(
        body,
        out_shape=[STACK, BUFFER, BUFFER, TOTALS],
        in_specs=[SMEM] + [VMEM] * (n_all + 3),
        out_specs=[VMEM] * 4,
        input_output_aliases={n_all + 2: 1, n_all + 3: 2, n_all + 1: 3},
        compiler_params=PARAMS,
        name="square_late",
    )(lists, *left_arrays, *right_arrays, totals, lbuf, rbuf)
    return out[0], out[2]


def cube_late(lists, totals, lbuf, rbuf, left, square):
    left_arrays, left_pieces = split(left)
    n_left = len(left_arrays)

    def body(plan_ref, *refs):
        _, _, rbuf, square_ref, out_ref, lbuf, total = refs[n_left:]
        fill(left_pieces, refs[:n_left], lbuf)
        for s in range(SLOTS):
            products(3, plan_ref, lbuf, rbuf, total.at[s], s)
            result = 3.0 * square_ref[s].astype(jnp.float32) - 2.0 * total[s]
            out_ref[plan_ref[ORDERS + s]] = result.astype(jnp.bfloat16)

    return pl.pallas_call(
        body,
        out_shape=[STACK, BUFFER, TOTALS],
        in_specs=[SMEM] + [VMEM] * (n_left + 4),
        out_specs=[VMEM] * 3,
        input_output_aliases={n_left + 2: 1, n_left + 1: 2},
        compiler_params=PARAMS,
        name="cube_late",
    )(lists, *left_arrays, totals, lbuf, rbuf, square)[0]


def parted(pieces, late):
    return [piece for piece in pieces if not late >> piece[0] & 1], [piece for piece in pieces if late >> piece[0] & 1]


def local(tiles, stack_index, block_mask):
    order, own = arrange(tiles[0, 0], stack_index[0, 0], block_mask)
    table = tables(block_mask)
    lists = plan(*table, order)
    right, partner = gather_rows(own)
    left = gather_cols(own, partner)
    right[0] = left[0]
    left, last_left = parted(left, LATE_COLS_FIRST)
    right, last_right = parted(right, LATE_ROWS)
    totals, lbuf, rbuf = multiply_early(0, lists, left, right)
    square, rbuf = square_late(lists, totals, lbuf, rbuf, last_left, last_right)
    left, last_left = parted(gather_cols(square), LATE_COLS_SECOND)
    totals, lbuf = multiply_early(2, lists, left, rbuf)
    purified = cube_late(lists, totals, lbuf, rbuf, last_left, square)
    return purified[None, None]


def solution(mesh):
    return jax.shard_map(
        local,
        mesh=mesh,
        in_specs=(P("row", "col", None, None, None), P("row", "col", None), P()),
        out_specs=P("row", "col", None, None, None),
        check_vma=False,
    )
```

```python
import jax
import jax.numpy as jnp
from jax import lax
from jax.experimental import pallas as pl
from jax.experimental.pallas import tpu as pltpu
from jax.sharding import PartitionSpec as P


NB = 64
BS = 256
HALF = BS // 2
SLOTS = 3
I32 = jnp.int32


def links():
    def table(move):
        pairs = []
        for z in range(8):
            for a in range(2):
                for b in range(2):
                    for y in range(4):
                        for c in range(2):
                            z2, a2, b2, y2, c2 = move(z, a, b, y, c)
                            here = (z * 2 + a) * 16 + b * 8 + y * 2 + c
                            there = (z2 % 8 * 2 + a2) * 16 + b2 * 8 + y2 % 4 * 2 + c2
                            pairs.append((here, there))
        return pairs

    def across(z, a, b, y, c):
        x = (b * 2 + a + (1 if a == 1 else -1)) % 4
        return z, x % 2, x // 2, y, c

    return {
        "z+": table(lambda z, a, b, y, c: (z - 1, a, b, y, c)),
        "z-": table(lambda z, a, b, y, c: (z + 1, a, b, y, c)),
        "y": table(lambda z, a, b, y, c: (z, a, b, y + (1 if c else -1), c)),
        "y2": table(lambda z, a, b, y, c: (z, a, b, y + 2, c)),
        "xl": table(lambda z, a, b, y, c: (z, 1 - a, b, y, c)),
        "xr": table(across),
        "xh": table(lambda z, a, b, y, c: (z, a, 1 - b, y, c)),
        "core": table(lambda z, a, b, y, c: (z, a, b, y, 1 - c)),
    }


LINKS = links()


def send(part, link):
    return lax.ppermute(part, ("row", "col"), LINKS[link])


LATE_ROWS = 1 << 11 | 1 << 12 | 1 << 13
LATE_COLS_FIRST = 1 << 11 | 1 << 14 | 1 << 15
LATE_COLS_SECOND = 1 << 9 | 1 << 11 | 1 << 13 | 1 << 15
STRIDE = 72
SPARE = SLOTS * 16
COUNTS = 4 * SLOTS * STRIDE
ORDERS = COUNTS + 16


def gather_rows(own):
    down1, up1 = send(own, "z-"), send(own, "z+")
    partner = send(own, "xl")
    down2, up2 = send(down1, "z-"), send(up1, "z+")
    across7, across1 = send(down1, "xl"), send(up1, "xl")
    down3, up3 = send(down2, "z-"), send(up2, "z+")
    across2, across6 = send(up2, "xl"), send(across7, "z-")
    up4 = [send(up3[:, row : row + HALF], "z+") for row in (0, HALF)]
    across5, across3 = send(across6, "z-"), send(across2, "z+")
    across4 = [send(part, "xl") for part in up4]
    stacks = [own, up1, up2, up3, None, down3, down2, down1]
    stacks += [partner, across1, across2, across3, None, across5, across6, across7]
    pieces = [(place, 0, stack) for place, stack in enumerate(stacks) if stack is not None]
    pieces += [(4, 0, up4[0]), (4, HALF, up4[1]), (12, 0, across4[0]), (12, HALF, across4[1])]
    return pieces, partner


def gather_cols(own, partner=None):
    twin = send(own, "core")
    both = jnp.concatenate([own, twin])
    near = send(both, "y")
    far = send(near, "core")
    opposite = send(own, "y2")
    opposite_twin = send(opposite, "core")
    if partner is None:
        x = send(own, "xh")
        x_opposite = send(opposite, "xh")
    else:
        x = send(partner, "xr")
        x_opposite = send(x, "y2")
    x_twin = send(x, "core")
    x_both = jnp.concatenate([x, x_twin])
    x_near = send(x_both, "y")
    x_far = send(x_near, "core")
    x_opposite_twin = send(x_opposite, "core")
    return [
        (0, 0, both), (4, SLOTS, both), (1, 0, near), (5, SLOTS, near), (7, 0, far), (3, SLOTS, far),
        (2, 0, opposite), (6, 0, opposite_twin), (8, 0, x_both), (12, SLOTS, x_both), (9, 0, x_near), (13, SLOTS, x_near),
        (15, 0, x_far), (11, SLOTS, x_far), (10, 0, x_opposite), (14, 0, x_opposite_twin),
    ]


SMEM = pl.BlockSpec(memory_space=pltpu.SMEM)
VMEM = pl.BlockSpec(memory_space=pltpu.VMEM)


def small(kib):
    return pltpu.CompilerParams(vmem_limit_bytes=kib * 1024)


def arrange(tiles, ids, mask):
    def body(ids_ref, mask_ref, tiles_ref, order_ref, own_ref):
        r, c = lax.axis_index("row"), lax.axis_index("col")
        keys = []
        for s in range(SLOTS):
            block = ids_ref[s]
            live = mask_ref[4 * r + block // 4, 4 * c + block % 4] > 0
            keys.append(jnp.where(live, block, 16 + s))
        for s in range(SLOTS):
            rank = sum((keys[t] < keys[s]).astype(I32) for t in range(SLOTS) if t != s)
            order_ref[rank] = s
            order_ref[SLOTS + rank] = ids_ref[s]
            own_ref[rank] = tiles_ref[s]
        order_ref[2 * SLOTS] = sum((key < 16).astype(I32) for key in keys)

    return pl.pallas_call(
        body,
        out_shape=(jax.ShapeDtypeStruct((8,), I32), jax.ShapeDtypeStruct((SLOTS, BS, BS), jnp.bfloat16)),
        in_specs=[SMEM, SMEM, VMEM],
        out_specs=(SMEM, VMEM),
        name="arrange",
    )(ids, mask, tiles)


def tables(mask):
    def body(mask_ref, left_ref, right_ref):
        r, c = lax.axis_index("row"), lax.axis_index("col")
        toward = jnp.where(c % 2 == 0, 1, 3)
        full = (mask_ref[...] > 0).astype(jnp.bfloat16)
        sub = lax.broadcasted_iota(I32, (8, NB), 0)
        lane = lax.broadcasted_iota(I32, (8, NB), 1)

        def dot(one, two, dims):
            return lax.dot_general(one, two, (dims, ((), ())), preferred_element_type=jnp.float32)

        rows = dot(((lane == 4 * r + sub) & (sub < 4)).astype(jnp.bfloat16), full, ((1,), (0,)))
        cols = dot(((lane == 4 * c + sub) & (sub < 4)).astype(jnp.bfloat16), full, ((1,), (1,)))
        k0 = lax.broadcasted_iota(I32, (NB, NB), 0)
        k1 = lax.broadcasted_iota(I32, (NB, NB), 1)
        same = (k0 >> 2) == (k1 >> 2)
        earlier = (same & (k0 < k1)).astype(jnp.bfloat16)
        above = (lax.broadcasted_iota(I32, (8, 8), 1) < lax.broadcasted_iota(I32, (8, 8), 0)).astype(jnp.bfloat16)
        rows16, cols16 = rows.astype(jnp.bfloat16), cols.astype(jnp.bfloat16)
        row_totals = dot(rows16, same.astype(jnp.bfloat16), ((1,), (0,))).astype(jnp.bfloat16)
        left_slot = dot(rows16, earlier, ((1,), (0,))) + dot(above, row_totals, ((1,), (0,)))
        col_totals = dot(jnp.ones((8, 8), jnp.bfloat16), cols16, ((1,), (0,))).astype(jnp.bfloat16)
        right_slot = dot(col_totals, earlier, ((1,), (0,))) + dot(above, cols16, ((1,), (0,)))

        k = lane >> 2
        left = ((((k >> 1) - (c // 2) + 16) & 3) * toward & 3) + 4 * ((k ^ c) & 1) + 8 * ((k >> 3) ^ (c // 8))
        right = (((k >> 1) - (r // 2) + 8) & 7) + 8 * ((k ^ r) & 1)

        def late(places, bits):
            return sum((places == place).astype(I32) for place in range(16) if bits >> place & 1)

        left_at = left * SLOTS + 64 * late(left, LATE_COLS_FIRST) + 128 * late(left, LATE_COLS_SECOND)
        right_at = right * SLOTS + 64 * late(right, LATE_ROWS)
        left_ref[...] = jnp.where(rows > 0.5, left_at + left_slot.astype(I32), -1)
        right_ref[...] = jnp.where(cols > 0.5, right_at + right_slot.astype(I32), -1)

    return pl.pallas_call(
        body,
        out_shape=(jax.ShapeDtypeStruct((8, NB), I32), jax.ShapeDtypeStruct((8, NB), I32)),
        in_specs=[VMEM],
        out_specs=(VMEM, VMEM),
        compiler_params=small(1024),
        name="tables",
    )(mask)


def plan(left_table, right_table, order):
    def body(left_ref, right_ref, order_ref, plan_ref):
        for s in range(SLOTS):
            plan_ref[ORDERS + s] = order_ref[s]
            block = order_ref[SLOTS + s]
            a, b = block // 4, block % 4

            def term(step, counts, a=a, b=b, s=s):
                for i in range(4):
                    k = 4 * step + i
                    left, right = left_ref[a, k], right_ref[b, k]
                    one = ((left >= 0) & (right >= 0)).astype(I32)
                    code = (left & 63) * 64 + (right & 63)
                    fresh = []
                    for first, late in ((0, ((left | right) >> 6) & 1), (2, (left >> 7) & 1)):
                        at = jnp.where(late > 0, counts[first + 1] + SLOTS * STRIDE, counts[first])
                        plan_ref[(first * SLOTS + s) * STRIDE + at] = code
                        more = one & late
                        fresh += [counts[first] + (one - more), counts[first + 1] + more]
                    counts = tuple(fresh)
                return counts

            zero = jnp.int32(0)
            counts = lax.fori_loop(0, jnp.where(s < order_ref[2 * SLOTS], NB // 4, 0), term, (zero, zero, zero, zero))
            for q in range(4):
                plan_ref[COUNTS + q * 4 + s] = counts[q]
                plan_ref[(q * SLOTS + s) * STRIDE + counts[q]] = SPARE * 65

    return pl.pallas_call(
        body,
        out_shape=jax.ShapeDtypeStruct((ORDERS + 8,), I32),
        in_specs=[SMEM, SMEM, SMEM],
        out_specs=SMEM,
        compiler_params=small(1024),
        name="plan",
    )(left_table, right_table, order)


def fill(pieces, refs, buf):
    for (place, first, _), which in zip(*pieces):
        source = refs[which]
        for s in range(SLOTS):
            if source.shape[1] == HALF:
                buf[place * SLOTS + s, pl.ds(first, HALF)] = source[s]
            else:
                buf[place * SLOTS + s] = source[first + s]


def split(pieces):
    arrays = list({id(array): array for _, _, array in pieces}.values())
    return arrays, (pieces, [[array is a for a in arrays].index(True) for _, _, array in pieces])


def products(which_list, plan_ref, lbuf, rbuf, total, s):
    def step(p, _):
        at = (which_list * SLOTS + s) * STRIDE + 2 * p
        one, two = plan_ref[at], plan_ref[at + 1]
        total[...] += jnp.dot(lbuf[one // 64], rbuf[one % 64], preferred_element_type=jnp.float32) + jnp.dot(
            lbuf[two // 64], rbuf[two % 64], preferred_element_type=jnp.float32
        )
        return 0

    lax.fori_loop(0, (plan_ref[COUNTS + which_list * 4 + s] + 1) // 2, step, 0)


BUFFER = jax.ShapeDtypeStruct((SPARE + 1, BS, BS), jnp.bfloat16)
TOTALS = jax.ShapeDtypeStruct((SLOTS, BS, BS), jnp.float32)
STACK = jax.ShapeDtypeStruct((SLOTS, BS, BS), jnp.bfloat16)
PARAMS = pltpu.CompilerParams(vmem_limit_bytes=8 * 1024 * 1024)


def multiply_early(which_list, lists, left, right):
    left_arrays, left_pieces = split(left)
    right_arrays, right_pieces = split(right) if isinstance(right, list) else ([right], None)
    n_left = len(left_arrays)

    def body(plan_ref, *refs):
        left_refs, right_refs, outs = refs[:n_left], refs[n_left : n_left + len(right_arrays)], refs[n_left + len(right_arrays) :]
        totals, lbuf = outs[:2]
        lbuf[SPARE] = jnp.zeros((BS, BS), jnp.bfloat16)
        fill(left_pieces, left_refs, lbuf)
        if right_pieces is None:
            rbuf = right_refs[0]
        else:
            rbuf = outs[2]
            rbuf[SPARE] = jnp.zeros((BS, BS), jnp.bfloat16)
            fill(right_pieces, right_refs, rbuf)
        for s in range(SLOTS):
            totals[s] = jnp.zeros((BS, BS), jnp.float32)
            products(which_list, plan_ref, lbuf, rbuf, totals.at[s], s)

    return pl.pallas_call(
        body,
        out_shape=[TOTALS, BUFFER] + ([] if right_pieces is None else [BUFFER]),
        in_specs=[SMEM] + [VMEM] * (n_left + len(right_arrays)),
        out_specs=[VMEM] * (2 if right_pieces is None else 3),
        compiler_params=PARAMS,
    )(lists, *left_arrays, *right_arrays)


def square_late(lists, totals, lbuf, rbuf, left, right):
    left_arrays, left_pieces = split(left)
    right_arrays, right_pieces = split(right)
    n_left, n_all = len(left_arrays), len(left_arrays) + len(right_arrays)

    def body(plan_ref, *refs):
        out_ref, lbuf, rbuf, total = refs[n_all + 3 :]
        fill(left_pieces, refs[:n_left], lbuf)
        fill(right_pieces, refs[n_left:n_all], rbuf)
        for s in range(SLOTS):
            products(1, plan_ref, lbuf, rbuf, total.at[s], s)
            out_ref[s] = total[s].astype(jnp.bfloat16)

    out = pl.pallas_call(
        body,
        out_shape=[STACK, BUFFER, BUFFER, TOTALS],
        in_specs=[SMEM] + [VMEM] * (n_all + 3),
        out_specs=[VMEM] * 4,
        input_output_aliases={n_all + 2: 1, n_all + 3: 2, n_all + 1: 3},
        compiler_params=PARAMS,
        name="square_late",
    )(lists, *left_arrays, *right_arrays, totals, lbuf, rbuf)
    return out[0], out[2]


def cube_late(lists, totals, lbuf, rbuf, left, square):
    left_arrays, left_pieces = split(left)
    n_left = len(left_arrays)

    def body(plan_ref, *refs):
        _, _, rbuf, square_ref, out_ref, lbuf, total = refs[n_left:]
        fill(left_pieces, refs[:n_left], lbuf)
        for s in range(SLOTS):
            products(3, plan_ref, lbuf, rbuf, total.at[s], s)
            result = 3.0 * square_ref[s].astype(jnp.float32) - 2.0 * total[s]
            out_ref[plan_ref[ORDERS + s]] = result.astype(jnp.bfloat16)

    return pl.pallas_call(
        body,
        out_shape=[STACK, BUFFER, TOTALS],
        in_specs=[SMEM] + [VMEM] * (n_left + 4),
        out_specs=[VMEM] * 3,
        input_output_aliases={n_left + 2: 1, n_left + 1: 2},
        compiler_params=PARAMS,
        name="cube_late",
    )(lists, *left_arrays, totals, lbuf, rbuf, square)[0]


def parted(pieces, late):
    return [piece for piece in pieces if not late >> piece[0] & 1], [piece for piece in pieces if late >> piece[0] & 1]


def local(tiles, stack_index, block_mask):
    order, own = arrange(tiles[0, 0], stack_index[0, 0], block_mask)
    table = tables(block_mask)
    lists = plan(*table, order)
    right, partner = gather_rows(own)
    left = gather_cols(own, partner)
    right[0] = left[0]
    left, last_left = parted(left, LATE_COLS_FIRST)
    right, last_right = parted(right, LATE_ROWS)
    totals, lbuf, rbuf = multiply_early(0, lists, left, right)
    square, rbuf = square_late(lists, totals, lbuf, rbuf, last_left, last_right)
    left, last_left = parted(gather_cols(square), LATE_COLS_SECOND)
    totals, lbuf = multiply_early(2, lists, left, rbuf)
    purified = cube_late(lists, totals, lbuf, rbuf, last_left, square)
    return purified[None, None]


def solution(mesh):
    return jax.shard_map(
        local,
        mesh=mesh,
        in_specs=(P("row", "col", None, None, None), P("row", "col", None), P()),
        out_specs=P("row", "col", None, None, None),
        check_vma=False,
    )
```
